32 devices in a mesh: band: 16 (over z, y, core), sub: 2 (over x).
Axes of the slice: x: 2, y: 2, z: 4, core: 2. Of those that a mesh axis runs over, the one named last changes fastest.
Arguments:
- land_values: bfloat16 [64, 524288], P(None, ('band', 'sub')), may hold values from -6 to 6
- area_weights: bfloat16 [4096, 128, 128], P(('band', 'sub')), may hold values from 0.0019989014 to 0.029907227
- land_mask: int32 [524288], P(('band', 'sub')), may hold values 0 or 1
- dest_band: int32 [4096, 1], P(('band', 'sub')), may hold values from 0 to 15; in each aligned block of 128 rows (0 to 127, 128 to 255, ...) at most 16 rows name the same one
- dest_tile: int32 [4096], P(('band', 'sub')), may hold values from 0 to 399
- ocean_mask: int32 [819200], P(('band', 'sub')), may hold values 0 or 1
Outputs:
- remapped: float32 [64, 819200], P(None, ('band', 'sub'))
The draws below stay inside these ranges and needn't reach their ends.
Inputs may be any that keep to these rules, and one draw needn't show every extreme that they name: `dest_band`: each device's 128 blocks name any one band at most 16 times; in every draw some device names one band exactly 16 times.
All inputs are finite; a program needn't handle non-finite values. No bound on the sum of `land_mask` or of `ocean_mask` on one device may be relied on, other than what follows from the above.
Results may differ from the reference program's by a relative error of at most 0.005.
Values may be sent and summed in bfloat16 or wider, within the bound.
No kernel may reach another device: no remote copies, remote signals or barrier semaphores. Data moves between devices by JAX's collectives and lax.ppermute only.
A program may use at most 128 MiB of HBM per device.

```python
import math
import jax
import jax.numpy as jnp
import numpy as np
from jax import lax

F = 64
BL = 128
OT = 128
LB_DEV = 128
CAP = 16
TILES_BAND = 400
NBLK = 4096
NLAND = 524288
NOCN = 819200
N_BAND = 16


def touch_ends(result, rng, low, largest):
    longest = result.shape.index(max(result.shape))
    spots = []
    for shift in (0, 1):
        where = [jax.random.randint(jax.random.fold_in(rng, axis), (), 0, length) for axis, length in enumerate(result.shape)]
        where[longest] = (where[longest] + shift) % result.shape[longest]
        spots.append(tuple(where))
    return result.at[spots[0]].set(low).at[spots[1]].set(largest)


def level_of(stream_key, shape, split, least, largest):
    def one(position, shards_of):
        draws = jax.random.uniform(jax.random.fold_in(jax.random.fold_in(stream_key, 6), position), (shards_of,), jnp.float32, least / len(split), largest / len(split))
        return jnp.repeat(jnp.exp(draws), shape[position] // shards_of).reshape((-1,) + (1,) * (len(shape) - position - 1))

    gain = one(*split[0])
    for cut in split[1:]:
        gain = gain * one(*cut)
    return gain


def shared_out(own_key, own, number, rows, number_of, top, bound, lean):
    sequence = jax.random.permutation(own_key, number_of)
    packed, common = load_shares(number_of, rows * top, bound, lean, True), load_shares(number_of, rows * top, bound, lean, False)
    places = jnp.arange(number_of)

    def named(tallies, offset_by):
        used = int((tallies > 0).sum())
        fixed = max(1, used // 4)
        shifted = fixed + (places - fixed + offset_by * (used - fixed)) % max(1, number_of - fixed)
        return jnp.zeros((number_of,), jnp.int32).at[sequence[jnp.where(places < fixed, places, shifted)]].set(jnp.asarray(tallies, jnp.int32))

    tallies = jnp.where(number % 4 == 0, named(packed, number // 4), named(common, number - number // 4 - 1))
    mixed = jax.random.permutation(jax.random.fold_in(own, 3), number_of)
    donor, sink = mixed[0:number_of // 2 * 2:2], mixed[1:number_of // 2 * 2:2]
    room = jnp.minimum(tallies[donor] - 1, bound - tallies[sink]) // 2
    room = jnp.where((donor == sequence[0]) | (sink == sequence[0]) | (tallies[sink] == 0), 0, jnp.maximum(room, 0))
    shifted = jax.random.randint(jax.random.fold_in(own, 4), (number_of // 2,), 0, 1 << 20) % (room + 1)
    tallies = tallies.at[donor].add(-shifted).at[sink].add(shifted)
    labels = jnp.searchsorted(jnp.cumsum(tallies), jnp.arange(rows * top), side="right").astype(jnp.int32)
    listing = labels.reshape(top, rows).T
    listing = listing[jax.random.permutation(jax.random.fold_in(own, 1), rows)]
    offset_by = jax.random.randint(jax.random.fold_in(own, 2), (rows, 1), 0, top)
    return jnp.take_along_axis(listing, (jnp.arange(top)[None, :] + offset_by) % top, axis=1)


def load_shares(count, total, reach, lean, full):
    loads = [(1 << 20) // math.isqrt(rank ** lean) + 1 for rank in range(1, count + 1)]
    largest = reach if full else min(reach, max(-(-total // count), total * loads[0] // sum(loads)))
    least = 1 if total - largest >= count - 1 else 0
    given, surplus = [largest] + [least] * (count - 1), total - largest - least * (count - 1)
    while surplus > 0:
        free = [i for i in range(1, count) if given[i] < largest] or [i for i in range(1, count) if given[i] < reach]
        pool, budget = sum([loads[i] for i in free]), surplus
        for i in free:
            more = min(reach - given[i], max(1, budget * loads[i] // pool), surplus)
            given[i] = given[i] + more
            surplus = surplus - more
    return np.array(given)


def gaussian(stream_key, dims, spread, most, shards=(), dtype=jnp.bfloat16):
    drawn = jax.random.normal(stream_key, dims, jnp.float32) * spread
    if len(shards) > 0:
        drawn = level_of(stream_key, dims, shards, -0.22, 0.18) * drawn
    return jnp.clip(drawn, min=-most, max=most).astype(dtype)


def setup_inputs(seed: int = 0) -> dict:
    key_of = jax.random.split(jax.random.key(seed), 7)
    land_values = gaussian(key_of[0], (F, NLAND), 1.0, 6.0, ((1, 32),))
    area_weights = jnp.clip(jnp.exp(math.log(0.029907227) - 2.7055024 * jax.random.uniform(key_of[1], (NBLK, BL, OT), jnp.float32) ** level_of(key_of[1], (NBLK, BL, OT), ((0, 32),), -0.2, 0.2)), 0.0019989014, 0.029907227).astype(jnp.bfloat16)
    land_mask = touch_ends((jax.random.randint(key_of[2], (NLAND,), 0, 2) < 1).astype(jnp.int32), jax.random.fold_in(key_of[2], 1), 0, 1)
    dest_band_keys = jax.random.split(jax.random.fold_in(key_of[3], 1), NBLK // LB_DEV)
    dest_band_turns = jax.random.permutation(jax.random.fold_in(key_of[3], 3), NBLK // LB_DEV)
    dest_band = jax.vmap(lambda own, number: shared_out(jax.random.fold_in(key_of[3], 2), own, number, LB_DEV, N_BAND, 1, CAP, 2))(dest_band_keys, dest_band_turns).reshape((NBLK, 1))
    dest_tile = touch_ends(jax.random.randint(key_of[4], (NBLK,), 0, TILES_BAND), jax.random.fold_in(key_of[4], 1), 0, TILES_BAND - 1).astype(jnp.int32)
    ocean_mask = touch_ends((jax.random.randint(key_of[5], (NOCN,), 0, 4) < 3).astype(jnp.int32), jax.random.fold_in(key_of[5], 1), 0, 1)
    return dict(land_values=land_values, area_weights=area_weights, land_mask=land_mask, dest_band=dest_band, dest_tile=dest_tile, ocean_mask=ocean_mask)


cover_floor = 0.5


def reference(land_values, area_weights, land_mask, dest_band, dest_tile, ocean_mask):
    groups = area_weights.shape[0] // LB_DEV
    tiles_all = N_BAND * TILES_BAND
    block_values = land_values.reshape(F, groups, LB_DEV, BL).transpose(1, 2, 0, 3)
    block_weights = area_weights.reshape(groups, LB_DEV, BL, OT)
    block_masks = land_mask.reshape(groups, LB_DEV, BL)
    block_tiles = (dest_band[:, 0] * TILES_BAND + dest_tile).astype(jnp.int32).reshape(groups, LB_DEV)

    def remap_group(carry, inputs):
        summed, coverage = carry
        values, weights, masks, tiles = inputs
        masked = weights * masks.astype(jnp.bfloat16)[:, :, None]
        partial_value = jnp.einsum("bfl,blo->bfo", values.astype(jnp.float32), masked.astype(jnp.float32)).astype(jnp.bfloat16)
        covered = jnp.sum(masked.astype(jnp.float32), axis=1).astype(jnp.bfloat16)
        summed = summed.at[:, tiles].add(jnp.transpose(partial_value.astype(jnp.float32), (1, 0, 2)))
        coverage = coverage.at[tiles].add(covered.astype(jnp.float32))
        return (summed, coverage), None

    start_state = (jnp.zeros((F, tiles_all, OT), jnp.float32), jnp.zeros((tiles_all, OT), jnp.float32))
    (summed, coverage), unused = lax.scan(remap_group, start_state, (block_values, block_weights, block_masks, block_tiles))
    ocean_keep = ocean_mask.reshape(tiles_all, OT).astype(jnp.float32)
    remapped = summed * ocean_keep[None] / jnp.maximum(coverage, cover_floor)[None]
    return remapped.reshape(F, tiles_all * OT)
```

```python
import functools

import jax
import jax.numpy as jnp
from jax import lax
from jax.experimental import pallas as pl
from jax.experimental.pallas import tpu as pltpu
from jax.sharding import PartitionSpec as P

cover_floor = 0.5
axes = ("band", "sub")
vmem_bytes = 56 * 1024 * 1024


def round_up(n, m):
    return -(-n // m) * m


def pick_chunk(total, wanted):
    for steps in range(wanted, 0, -1):
        if total % steps == 0:
            return total // steps
    return total


def pack_kernel(group, slots, owner_ref, slot_ref, values_ref, weights_ref, mask_ref, out_ref, cov_ref):
    step = pl.program_id(0)
    fields = values_ref.shape[0]
    cells = weights_ref.shape[1]

    @pl.when(step == 0)
    def _():
        out_ref[...] = jnp.zeros_like(out_ref)
        cov_ref[...] = jnp.zeros_like(cov_ref)

    keep = mask_ref[...].astype(jnp.float32).astype(jnp.bfloat16)
    for j in range(group):
        block = step * group + j
        owner = owner_ref[block]
        slot = slot_ref[block]
        row = keep[j : j + 1, :]
        kept = values_ref[:, j * cells : (j + 1) * cells] * row
        left = jnp.concatenate([kept, jnp.broadcast_to(row, (16, cells))], axis=0)
        both = jnp.dot(left, weights_ref[j], preferred_element_type=jnp.float32)
        out_ref[owner, pl.ds(pl.multiple_of(slot * fields, fields), fields), :] = both[:fields].astype(
            jnp.bfloat16
        )
        cov_ref[owner, pl.ds(slot, 1), :] = both[fields : fields + 1]

    @pl.when(step == pl.num_programs(0) - 1)
    def _():
        out_ref[:, slots * fields :, :] = cov_ref[...].astype(jnp.bfloat16)


def pack(owner, slot, values, weights, mask, n_dev, slots):
    fields = values.shape[0]
    blocks, cells, tile_cells = weights.shape
    group = pick_chunk(blocks, 8)
    rows = slots * fields + round_up(slots, 16)
    return pl.pallas_call(
        functools.partial(pack_kernel, group, slots),
        out_shape=jax.ShapeDtypeStruct((n_dev, rows, tile_cells), jnp.bfloat16),
        grid_spec=pltpu.PrefetchScalarGridSpec(
            num_scalar_prefetch=2,
            grid=(blocks // group,),
            in_specs=[
                pl.BlockSpec((fields, group * cells), lambda i, *_: (0, i)),
                pl.BlockSpec((group, cells, tile_cells), lambda i, *_: (i, 0, 0)),
                pl.BlockSpec((group, cells), lambda i, *_: (i, 0)),
            ],
            out_specs=pl.BlockSpec((n_dev, rows, tile_cells), lambda i, *_: (0, 0, 0)),
            scratch_shapes=[pltpu.VMEM((n_dev, round_up(slots, 16), tile_cells), jnp.float32)],
        ),
        compiler_params=pltpu.CompilerParams(vmem_limit_bytes=vmem_bytes),
        name="pack",
    )(owner, slot, values, weights, mask)


def pick_kernel(count, fields, slots, which_ref, recv_ref, out_ref, cov_in, cov_out):
    cov_in[...] = recv_ref[:, slots * fields :, :].astype(jnp.float32)
    cov_out[...] = jnp.zeros_like(cov_out)

    def one(k, carry):
        at = which_ref[k]
        src = at // slots
        slot = at % slots
        out_ref[pl.ds(pl.multiple_of(k * fields, fields), fields), :] = recv_ref[
            src, pl.ds(pl.multiple_of(slot * fields, fields), fields), :
        ]
        cov_out[pl.ds(k, 1), :] = cov_in[src, pl.ds(slot, 1), :]
        return carry

    lax.fori_loop(0, count, one, 0)
    out_ref[count * fields :, :] = cov_out[...].astype(jnp.bfloat16)


def pick(which, recv, count, fields, slots):
    n_dev, rows, tile_cells = recv.shape
    cov_rows = round_up(count, 16)
    return pl.pallas_call(
        functools.partial(pick_kernel, count, fields, slots),
        out_shape=jax.ShapeDtypeStruct((count * fields + cov_rows, tile_cells), jnp.bfloat16),
        in_specs=[
            pl.BlockSpec(memory_space=pltpu.SMEM),
            pl.BlockSpec(memory_space=pltpu.VMEM),
        ],
        out_specs=pl.BlockSpec(memory_space=pltpu.VMEM),
        scratch_shapes=[
            pltpu.VMEM((n_dev, rows - slots * fields, tile_cells), jnp.float32),
            pltpu.VMEM((cov_rows, tile_cells), jnp.float32),
        ],
        compiler_params=pltpu.CompilerParams(vmem_limit_bytes=vmem_bytes),
        name="pick",
    )(which, recv)


def place_kernel(
    count, slots, chunk, own_ref, late_ref, recv_ref, fix_ref, keep_ref, out_ref, acc, cover, cov_own, cov_fix
):
    step = pl.program_id(0)
    fields = out_ref.shape[0]
    cells = keep_ref.shape[1]
    tiles = keep_ref.shape[0]
    n_dev = recv_ref.shape[0]

    @pl.when(step == 0)
    def _():
        acc[...] = jnp.zeros_like(acc)
        cover[...] = jnp.zeros_like(cover)
        cov_own[...] = recv_ref[:, slots * fields :, :].astype(jnp.float32)
        cov_fix[...] = fix_ref[count * fields :, :].astype(jnp.float32)

        def own(src, carry):
            for k in range(slots):
                tile = own_ref[src * slots + k]
                acc[tile] += recv_ref[src, k * fields : (k + 1) * fields, :].astype(jnp.float32)
                cover[pl.ds(tile, 1), :] += cov_own[src, k : k + 1, :]
            return carry

        lax.fori_loop(0, n_dev, own, 0)

        def late(k, carry):
            tile = late_ref[k]
            acc[tile] += fix_ref[pl.ds(pl.multiple_of(k * fields, fields), fields), :].astype(jnp.float32)
            cover[pl.ds(tile, 1), :] += cov_fix[pl.ds(k, 1), :]
            return carry

        lax.fori_loop(0, count, late, 0)
        total = cover[:tiles, :]
        cover[:tiles, :] = keep_ref[...].astype(jnp.float32) / jnp.maximum(total, cover_floor)

    for j in range(chunk):
        tile = step * chunk + j
        out_ref[:, j * cells : (j + 1) * cells] = acc[tile] * cover[pl.ds(tile, 1), :]


def place(own, late, recv, fix, keep, count, fields, slots):
    n_dev, rows, cells = recv.shape
    tiles = keep.shape[0]
    chunk = pick_chunk(tiles, 8)
    cov_rows = round_up(count, 16)
    return pl.pallas_call(
        functools.partial(place_kernel, count, slots, chunk),
        out_shape=jax.ShapeDtypeStruct((fields, tiles * cells), jnp.float32),
        grid_spec=pltpu.PrefetchScalarGridSpec(
            num_scalar_prefetch=2,
            grid=(tiles // chunk,),
            in_specs=[
                pl.BlockSpec((n_dev, rows, cells), lambda i, *_: (0, 0, 0)),
                pl.BlockSpec(fix.shape, lambda i, *_: (0, 0)),
                pl.BlockSpec((tiles, cells), lambda i, *_: (0, 0)),
            ],
            out_specs=pl.BlockSpec((fields, chunk * cells), lambda i, *_: (0, i)),
            scratch_shapes=[
                pltpu.VMEM((tiles + 1, fields, cells), jnp.float32),
                pltpu.VMEM((round_up(tiles + 1, 8), cells), jnp.float32),
                pltpu.VMEM((n_dev, rows - slots * fields, cells), jnp.float32),
                pltpu.VMEM((cov_rows, cells), jnp.float32),
            ],
        ),
        compiler_params=pltpu.CompilerParams(vmem_limit_bytes=vmem_bytes),
        name="place",
    )(own, late, recv, fix, keep)


def compact(chosen, values, count, empty):
    order = jnp.arange(chosen.shape[0], dtype=jnp.int32)
    earlier = (order[None, :] < order[:, None]) & chosen[None, :]
    rank = jnp.sum(earlier.astype(jnp.int32), axis=1)
    hit = (jnp.arange(count, dtype=jnp.int32)[:, None] == rank[None, :]) & chosen[None, :]
    got = jnp.sum(jnp.where(hit, (values - empty)[None, :], 0), axis=1)
    return got + empty


def per_device(land_values, area_weights, land_mask, dest_band, dest_tile, ocean_mask):
    fields = land_values.shape[0]
    blocks_here, block_cells, tile_cells = area_weights.shape
    band_count = lax.axis_size("band")
    halves = lax.axis_size("sub")
    assert halves == 2
    n_dev = band_count * halves
    capacity = max(2, 2 * blocks_here // band_count)
    slots = -(-capacity // halves)
    n_slots = n_dev * slots
    tiles = ocean_mask.shape[0] // tile_cells
    me = lax.axis_index("sub")

    band = dest_band[:, 0]
    half = (dest_tile >= tiles).astype(jnp.int32)
    key = band * halves + half
    order = jnp.arange(blocks_here, dtype=jnp.int32)
    same = key[:, None] == key[None, :]
    rank = jnp.sum((same & (order[None, :] < order[:, None])).astype(jnp.int32), axis=1)
    other = key + 1 - 2 * half
    other_count = jnp.sum((other[:, None] == key[None, :]).astype(jnp.int32), axis=1)
    spill = rank >= slots
    owner = jnp.where(spill, other, key)
    slot = jnp.where(spill, other_count + rank - slots, rank)
    flat = owner * slots + slot

    placed = jnp.arange(n_slots, dtype=jnp.int32)[:, None] == flat[None, :]
    tile_sent = jnp.sum(jnp.where(placed, dest_tile[None, :] + 1, 0), axis=1) - 1
    tile_sent = tile_sent.reshape(band_count, 1, halves * slots)
    tile_sent = jnp.broadcast_to(tile_sent, (band_count, halves, halves * slots)).reshape(n_dev, halves * slots)
    spilled = (jnp.arange(n_dev, dtype=jnp.int32)[:, None] == owner[None, :]) & spill[None, :]
    spill_count = jnp.sum(spilled.astype(jnp.int32), axis=1)
    table = jnp.concatenate([tile_sent, jnp.broadcast_to(spill_count[None, :], (n_dev, n_dev))], axis=1)
    table = lax.all_to_all(table, axes, split_axis=0, concat_axis=0, tiled=True)

    packed = pack(
        owner, slot, land_values, area_weights, land_mask.reshape(blocks_here, block_cells), n_dev, slots
    )
    recv = lax.all_to_all(packed, axes, split_axis=0, concat_axis=0, tiled=True)

    both = table[:, : halves * slots].reshape(n_dev, halves, slots)
    mine = jnp.where(me == 0, both[:, 0], both[:, 1]).reshape(n_slots)
    theirs = jnp.where(me == 0, both[:, 1], both[:, 0]).reshape(n_slots)
    low = me * tiles
    mine_here = (mine >= low) & (mine < low + tiles)
    own = jnp.where(mine_here, mine - low, tiles)
    away = (mine >= 0) & ~mine_here
    arriving = (theirs >= low) & (theirs < low + tiles)
    most = jnp.max(jnp.sum(table[:, halves * slots :], axis=0))
    keep = ocean_mask.reshape(tiles, tile_cells)
    which = compact(away, jnp.arange(n_slots, dtype=jnp.int32), n_slots, 0)
    late = compact(arriving, theirs - low, n_slots, tiles)

    def finish(count):
        def run(recv, which, late, own, keep):
            fix = pick(which[:count], recv, count, fields, slots)
            fix = lax.ppermute(fix, "sub", [(0, 1), (1, 0)])
            return place(own, late[:count], recv, fix, keep, count, fields, slots)

        return run

    few = min(n_slots, round_up(3 * n_slots // 16, 16))
    return lax.cond(most <= few, finish(few), finish(n_slots), recv, which, late, own, keep)


def solution(mesh):
    in_specs = (
        P(None, axes),
        P(axes, None, None),
        P(axes),
        P(axes, None),
        P(axes),
        P(axes),
    )
    return jax.shard_map(
        per_device, mesh=mesh, in_specs=in_specs, out_specs=P(None, axes), check_vma=False
    )
```

```python
import functools

import jax
import jax.numpy as jnp
from jax import lax
from jax.experimental import pallas as pl
from jax.experimental.pallas import tpu as pltpu
from jax.sharding import PartitionSpec as P

cover_floor = 0.5
axes = ("band", "sub")
vmem_bytes = 56 * 1024 * 1024


def round_up(n, m):
    return -(-n // m) * m


def pick_chunk(total, wanted):
    for steps in range(wanted, 0, -1):
        if total % steps == 0:
            return total // steps
    return total


def pack_kernel(
    group, slots, owner_ref, slot_ref, values_ref, weights_ref, mask_ref, meta_ref, lead_ref, tail_ref, cov_ref
):
    step = pl.program_id(0)
    fields = values_ref.shape[0]
    cells = weights_ref.shape[1]
    last = tail_ref.shape[1] // slots
    first = fields - last

    @pl.when(step == 0)
    def _():
        lead_ref[...] = jnp.zeros_like(lead_ref)
        tail_ref[...] = jnp.zeros_like(tail_ref)
        cov_ref[...] = jnp.zeros_like(cov_ref)
        cov_ref[:, slots : slots + meta_ref.shape[1], :] = meta_ref[...]

    keep = mask_ref[...].astype(jnp.float32).astype(jnp.bfloat16)
    for j in range(group):
        block = step * group + j
        owner = owner_ref[block]
        slot = slot_ref[block]
        row = keep[j : j + 1, :]
        kept = values_ref[:, j * cells : (j + 1) * cells] * row
        left = jnp.concatenate([kept, jnp.broadcast_to(row, (16, cells))], axis=0)
        both = jnp.dot(left, weights_ref[j], preferred_element_type=jnp.float32)
        lead_ref[owner, pl.ds(pl.multiple_of(slot * first, 16), first), :] = both[:first].astype(jnp.bfloat16)
        tail_ref[owner, pl.ds(pl.multiple_of(slot * last, 16), last), :] = both[first:fields].astype(
            jnp.bfloat16
        )
        cov_ref[owner, pl.ds(slot, 1), :] = both[fields : fields + 1]

    @pl.when(step == pl.num_programs(0) - 1)
    def _():
        lead_ref[:, slots * first :, :] = cov_ref[...].astype(jnp.bfloat16)


def pack(owner, slot, values, weights, mask, meta, slots, last):
    n_dev, meta_rows = meta.shape[:2]
    cov_rows = round_up(slots + meta_rows, 16)
    fields = values.shape[0]
    blocks, cells, tile_cells = weights.shape
    group = pick_chunk(blocks, 8)
    lead = (n_dev, slots * (fields - last) + cov_rows, tile_cells)
    tail = (n_dev, slots * last, tile_cells)
    return pl.pallas_call(
        functools.partial(pack_kernel, group, slots),
        out_shape=(jax.ShapeDtypeStruct(lead, jnp.bfloat16), jax.ShapeDtypeStruct(tail, jnp.bfloat16)),
        grid_spec=pltpu.PrefetchScalarGridSpec(
            num_scalar_prefetch=2,
            grid=(blocks // group,),
            in_specs=[
                pl.BlockSpec((fields, group * cells), lambda i, *_: (0, i)),
                pl.BlockSpec((group, cells, tile_cells), lambda i, *_: (i, 0, 0)),
                pl.BlockSpec((group, cells), lambda i, *_: (i, 0)),
                pl.BlockSpec(meta.shape, lambda i, *_: (0, 0, 0)),
            ],
            out_specs=(
                pl.BlockSpec(lead, lambda i, *_: (0, 0, 0)),
                pl.BlockSpec(tail, lambda i, *_: (0, 0, 0)),
            ),
            scratch_shapes=[pltpu.VMEM((n_dev, cov_rows, tile_cells), jnp.float32)],
        ),
        compiler_params=pltpu.CompilerParams(vmem_limit_bytes=vmem_bytes),
        name="pack",
    )(owner, slot, values, weights, mask, meta)


def pick_kernel(count, fields, slots, which_ref, recv_ref, out_ref, cov_in, cov_out):
    with_cover = recv_ref.shape[1] > slots * fields
    if with_cover:
        cov_in[...] = recv_ref[:, slots * fields :, :].astype(jnp.float32)
        cov_out[...] = jnp.zeros_like(cov_out)

    def one(k, carry):
        at = which_ref[k]
        src = at // slots
        slot = at % slots
        out_ref[pl.ds(pl.multiple_of(k * fields, 16), fields), :] = recv_ref[
            src, pl.ds(pl.multiple_of(slot * fields, 16), fields), :
        ]
        if with_cover:
            cov_out[pl.ds(k, 1), :] = cov_in[src, pl.ds(slot, 1), :]
        return carry

    lax.fori_loop(0, count, one, 0)
    if with_cover:
        out_ref[count * fields :, :] = cov_out[...].astype(jnp.bfloat16)


def pick(which, recv, count, fields, slots):
    n_dev, rows, tile_cells = recv.shape
    cov_rows = round_up(count, 16)
    extra = cov_rows if rows > slots * fields else 0
    return pl.pallas_call(
        functools.partial(pick_kernel, count, fields, slots),
        out_shape=jax.ShapeDtypeStruct((count * fields + extra, tile_cells), jnp.bfloat16),
        in_specs=[
            pl.BlockSpec(memory_space=pltpu.SMEM),
            pl.BlockSpec(memory_space=pltpu.VMEM),
        ],
        out_specs=pl.BlockSpec(memory_space=pltpu.VMEM),
        scratch_shapes=[
            pltpu.VMEM((n_dev, max(8, rows - slots * fields), tile_cells), jnp.float32),
            pltpu.VMEM((cov_rows, tile_cells), jnp.float32),
        ],
        compiler_params=pltpu.CompilerParams(vmem_limit_bytes=vmem_bytes),
        name="pick",
    )(which, recv)


def place_kernel(
    count, slots, chunk, own_ref, late_ref, lead_ref, tail_ref, fix_lead_ref, fix_tail_ref, keep_ref,
    out_ref, acc, cover, cov_own, cov_fix,
):
    step = pl.program_id(0)
    fields = out_ref.shape[0]
    cells = keep_ref.shape[1]
    tiles = keep_ref.shape[0]
    n_dev = lead_ref.shape[0]
    last = tail_ref.shape[1] // slots
    first = fields - last

    @pl.when(step == 0)
    def _():
        acc[...] = jnp.zeros_like(acc)
        cover[...] = jnp.zeros_like(cover)
        cov_own[...] = lead_ref[:, slots * first :, :].astype(jnp.float32)
        cov_fix[...] = fix_lead_ref[count * first :, :].astype(jnp.float32)

        def own(src, carry):
            for k in range(slots):
                tile = own_ref[src * slots + k]
                acc[tile, :first] += lead_ref[src, k * first : (k + 1) * first, :].astype(jnp.float32)
                acc[tile, first:] += tail_ref[src, k * last : (k + 1) * last, :].astype(jnp.float32)
                cover[pl.ds(tile, 1), :] += cov_own[src, k : k + 1, :]
            return carry

        lax.fori_loop(0, n_dev, own, 0)

        def late(k, carry):
            tile = late_ref[k]
            lead = fix_lead_ref[pl.ds(pl.multiple_of(k * first, 16), first), :]
            tail = fix_tail_ref[pl.ds(pl.multiple_of(k * last, 16), last), :]
            acc[tile, :first] += lead.astype(jnp.float32)
            acc[tile, first:] += tail.astype(jnp.float32)
            cover[pl.ds(tile, 1), :] += cov_fix[pl.ds(k, 1), :]
            return carry

        lax.fori_loop(0, count, late, 0)
        total = cover[:tiles, :]
        cover[:tiles, :] = keep_ref[...].astype(jnp.float32) / jnp.maximum(total, cover_floor)

    for j in range(chunk):
        tile = step * chunk + j
        out_ref[:, j * cells : (j + 1) * cells] = acc[tile] * cover[pl.ds(tile, 1), :]


def place(own, late, lead, tail, fix_lead, fix_tail, keep, count, fields, slots):
    n_dev = lead.shape[0]
    tiles, cells = keep.shape
    chunk = pick_chunk(tiles, 8)
    whole = lambda x: pl.BlockSpec(x.shape, lambda i, *_: (0,) * x.ndim)
    return pl.pallas_call(
        functools.partial(place_kernel, count, slots, chunk),
        out_shape=pltpu.HBM((fields, tiles * cells), jnp.float32),
        grid_spec=pltpu.PrefetchScalarGridSpec(
            num_scalar_prefetch=2,
            grid=(tiles // chunk,),
            in_specs=[whole(lead), whole(tail), whole(fix_lead), whole(fix_tail), whole(keep)],
            out_specs=pl.BlockSpec((fields, chunk * cells), lambda i, *_: (0, i)),
            scratch_shapes=[
                pltpu.VMEM((tiles + 1, fields, cells), jnp.float32),
                pltpu.VMEM((round_up(tiles + 1, 8), cells), jnp.float32),
                pltpu.VMEM((n_dev, lead.shape[1] - slots * (fields - tail.shape[1] // slots), cells), jnp.float32),
                pltpu.VMEM((round_up(count, 16), cells), jnp.float32),
            ],
        ),
        compiler_params=pltpu.CompilerParams(vmem_limit_bytes=vmem_bytes),
        name="place",
    )(own, late, lead, tail, fix_lead, fix_tail, keep)


def compact(chosen, values, count, empty):
    order = jnp.arange(chosen.shape[0], dtype=jnp.int32)
    earlier = (order[None, :] < order[:, None]) & chosen[None, :]
    rank = jnp.sum(earlier.astype(jnp.int32), axis=1)
    hit = (jnp.arange(count, dtype=jnp.int32)[:, None] == rank[None, :]) & chosen[None, :]
    got = jnp.sum(jnp.where(hit, (values - empty)[None, :], 0), axis=1)
    return got + empty


def per_device(land_values, area_weights, land_mask, dest_band, dest_tile, ocean_mask):
    fields = land_values.shape[0]
    blocks_here, block_cells, tile_cells = area_weights.shape
    band_count = lax.axis_size("band")
    halves = lax.axis_size("sub")
    assert halves == 2
    n_dev = band_count * halves
    capacity = max(2, 2 * blocks_here // band_count)
    slots = -(-capacity // halves)
    n_slots = n_dev * slots
    tiles = ocean_mask.shape[0] // tile_cells
    me = lax.axis_index("sub")

    band = dest_band[:, 0]
    half = (dest_tile >= tiles).astype(jnp.int32)
    key = band * halves + half
    order = jnp.arange(blocks_here, dtype=jnp.int32)
    same = key[:, None] == key[None, :]
    rank = jnp.sum((same & (order[None, :] < order[:, None])).astype(jnp.int32), axis=1)
    other = key + 1 - 2 * half
    other_count = jnp.sum((other[:, None] == key[None, :]).astype(jnp.int32), axis=1)
    spill = rank >= slots
    owner = jnp.where(spill, other, key)
    slot = jnp.where(spill, other_count + rank - slots, rank)
    flat = owner * slots + slot

    placed = jnp.arange(n_slots, dtype=jnp.int32)[:, None] == flat[None, :]
    tile_sent = jnp.sum(jnp.where(placed, dest_tile[None, :] + 1, 0), axis=1)
    tile_sent = tile_sent.reshape(band_count, 1, halves * slots)
    tile_sent = jnp.broadcast_to(tile_sent, (band_count, halves, halves * slots)).reshape(n_dev, halves * slots)
    spilled = (jnp.arange(n_dev, dtype=jnp.int32)[:, None] == owner[None, :]) & spill[None, :]
    spill_count = jnp.sum(spilled.astype(jnp.int32), axis=1)
    count_rows = round_up(n_dev, tile_cells) // tile_cells
    pad = ((0, 0), (0, tile_cells - halves * slots))
    counts = jnp.pad(spill_count, (0, count_rows * tile_cells - n_dev)).reshape(1, count_rows, tile_cells)
    meta = jnp.concatenate(
        [
            jnp.pad(tile_sent // 128, pad)[:, None, :],
            jnp.pad(tile_sent % 128, pad)[:, None, :],
            jnp.broadcast_to(counts, (n_dev, count_rows, tile_cells)),
        ],
        axis=1,
    ).astype(jnp.float32)

    last = max(16, fields // 64 * 16)
    first = fields - last
    lead, tail = pack(
        owner,
        slot,
        land_values,
        area_weights,
        land_mask.reshape(blocks_here, block_cells),
        meta,
        slots,
        last,
    )
    lead = lax.all_to_all(lead, axes, split_axis=0, concat_axis=0, tiled=True)
    tail, lead = lax.optimization_barrier((tail, lead))
    tail = lax.all_to_all(tail, axes, split_axis=0, concat_axis=0, tiled=True)

    table = lead[:, slots * first + slots : slots * first + slots + 2 + count_rows, :].astype(jnp.int32)
    both = table[:, 0, : halves * slots] * 128 + table[:, 1, : halves * slots] - 1
    both = both.reshape(n_dev, halves, slots)
    mine = jnp.where(me == 0, both[:, 0], both[:, 1]).reshape(n_slots)
    theirs = jnp.where(me == 0, both[:, 1], both[:, 0]).reshape(n_slots)
    low = me * tiles
    mine_here = (mine >= low) & (mine < low + tiles)
    own = jnp.where(mine_here, mine - low, tiles)
    away = (mine >= 0) & ~mine_here
    arriving = (theirs >= low) & (theirs < low + tiles)
    most = jnp.max(jnp.sum(table[:, 2:, :], axis=0))
    keep = ocean_mask.reshape(tiles, tile_cells)
    which = compact(away, jnp.arange(n_slots, dtype=jnp.int32), n_slots, 0)
    late = compact(arriving, theirs - low, n_slots, tiles)

    def hand_over(received, count, width):
        chosen = pick(which[:count], received, count, width, slots)
        return lax.ppermute(chosen, "sub", [(0, 1), (1, 0)])

    few = min(n_slots, round_up(3 * n_slots // 16, 16))
    fix_lead = hand_over(lead, few, first)
    fix_tail = hand_over(tail, few, last)

    def all_fit():
        return place(own, late[:few], lead, tail, fix_lead, fix_tail, keep, few, fields, slots)

    def redo():
        return place(
            own,
            late,
            lead,
            tail,
            hand_over(lead, n_slots, first),
            hand_over(tail, n_slots, last),
            keep,
            n_slots,
            fields,
            slots,
        )

    return lax.cond(most <= few, all_fit, redo)


def solution(mesh):
    in_specs = (
        P(None, axes),
        P(axes, None, None),
        P(axes),
        P(axes, None),
        P(axes),
        P(axes),
    )
    return jax.shard_map(
        per_device, mesh=mesh, in_specs=in_specs, out_specs=P(None, axes), check_vma=False
    )
```
